8 devices in a mesh: dp: 1 (over z), tp: 2 (over y), sp: 4 (over x, core).
Axes of the slice: x: 2, y: 2, z: 1, core: 2. Of those that a mesh axis runs over, the one named last changes fastest.
Arguments:
- x_seq: bfloat16 [6144, 2304], P(('dp', 'sp', 'tp'))
- w_query: bfloat16 [2304, 8, 256], P(None, 'tp')
- w_key: bfloat16 [2304, 4, 256], P(None, 'tp')
- w_value: bfloat16 [2304, 4, 256], P(None, 'tp')
- w_out: bfloat16 [8, 256, 2304], P('tp')
Outputs:
- output: bfloat16 [6144, 2304], P(('dp', 'sp', 'tp'))
All inputs are finite; a program needn't handle non-finite values.
Results may differ from the reference program's by a relative error of at most 0.00556017.
Values are sent between devices in bfloat16 or wider.
A program may use at most 1 GiB of HBM per device.

```python
import jax
import jax.numpy as jnp
from jax import lax

D = 2304
HEADS = 8
KV_HEADS = 4
HEAD = 256
WINDOW = 4096
CHUNK = 768
SP = 4
QBLOCK = 128

SEQ = 2 * SP * CHUNK
GROUP = HEADS // KV_HEADS
SPAN = WINDOW + QBLOCK
NEG_BIG = -1e30


def setup_inputs(seed: int = 0, part: int = 0) -> dict:
    base_key = jax.random.key(seed)
    part_key = jax.random.fold_in(base_key, part)
    weight_keys = jax.random.split(base_key, 4)
    x_rows = jax.random.normal(part_key, (SEQ, D), jnp.float32)
    w_query = jax.random.normal(weight_keys[0], (D, HEADS, HEAD), jnp.float32) * (1.5 * D ** -0.5)
    w_key = jax.random.normal(weight_keys[1], (D, KV_HEADS, HEAD), jnp.float32) * D ** -0.5
    w_value = jax.random.normal(weight_keys[2], (D, KV_HEADS, HEAD), jnp.float32) * D ** -0.5
    w_out = jax.random.normal(weight_keys[3], (HEADS, HEAD, D), jnp.float32) * (HEADS * HEAD) ** -0.5
    return {"x_seq": x_rows.astype(jnp.bfloat16), "w_query": w_query.astype(jnp.bfloat16), "w_key": w_key.astype(jnp.bfloat16), "w_value": w_value.astype(jnp.bfloat16), "w_out": w_out.astype(jnp.bfloat16)}


def to_natural(rows_in):
    blocks = rows_in.reshape((SP, 2, CHUNK) + rows_in.shape[1:])
    return jnp.concatenate([blocks[:, 0], blocks[::-1, 1]], axis=0).reshape(rows_in.shape)


def to_stored(rows_in):
    blocks = rows_in.reshape((2 * SP, CHUNK) + rows_in.shape[1:])
    return jnp.stack([blocks[:SP], blocks[SP:][::-1]], axis=1).reshape(rows_in.shape)


def reference(x_seq, w_query, w_key, w_value, w_out):
    x_nat = to_natural(x_seq)
    q_all = jnp.dot(x_nat, w_query.reshape(D, HEADS * HEAD), preferred_element_type=jnp.float32).astype(jnp.bfloat16).reshape(SEQ, KV_HEADS, GROUP, HEAD)
    k_all = jnp.dot(x_nat, w_key.reshape(D, KV_HEADS * HEAD), preferred_element_type=jnp.float32).astype(jnp.bfloat16).reshape(SEQ, KV_HEADS, HEAD)
    v_all = jnp.dot(x_nat, w_value.reshape(D, KV_HEADS * HEAD), preferred_element_type=jnp.float32).astype(jnp.bfloat16).reshape(SEQ, KV_HEADS, HEAD)
    zero_front = jnp.zeros((WINDOW, KV_HEADS, HEAD), jnp.bfloat16)
    k_pad = jnp.concatenate([zero_front, k_all], axis=0)
    v_pad = jnp.concatenate([zero_front, v_all], axis=0)
    score_scale = HEAD ** -0.5
    row_ids = jnp.arange(QBLOCK)[:, None]
    col_ids = jnp.arange(SPAN)[None, :]

    def one_block(start):
        q_blk = lax.dynamic_slice_in_dim(q_all, start, QBLOCK, 0).astype(jnp.float32)
        k_blk = lax.dynamic_slice_in_dim(k_pad, start, SPAN, 0).astype(jnp.float32)
        v_blk = lax.dynamic_slice_in_dim(v_pad, start, SPAN, 0).astype(jnp.float32)
        scores = jnp.einsum("qhgd,khd->hgqk", q_blk, k_blk) * score_scale
        pos_gap = WINDOW + row_ids - col_ids
        visible = (pos_gap >= 0) & (pos_gap < WINDOW) & (start - WINDOW + col_ids >= 0)
        scores = jnp.where(visible, scores, NEG_BIG)
        row_max = jnp.max(scores, axis=-1, keepdims=True)
        prob_blk = jnp.where(visible, jnp.exp(scores - row_max), 0.0)
        row_denom = jnp.sum(prob_blk, axis=-1)
        weighted = jnp.einsum("hgqk,khd->hgqd", prob_blk.astype(jnp.bfloat16).astype(jnp.float32), v_blk)
        normed = (weighted / row_denom[..., None]).astype(jnp.bfloat16)
        return jnp.transpose(normed, (2, 0, 1, 3)).reshape(QBLOCK, HEADS * HEAD)

    starts = jnp.arange(SEQ // QBLOCK) * QBLOCK
    o_nat = lax.map(one_block, starts).reshape(SEQ, HEADS * HEAD)
    y_nat = jnp.dot(o_nat, w_out.reshape(HEADS * HEAD, D), preferred_element_type=jnp.float32).astype(jnp.bfloat16)
    return to_stored(y_nat)
```

```python
import functools

import jax
import jax.numpy as jnp
from jax import lax
from jax.experimental import pallas as pl
from jax.experimental.pallas import tpu as pltpu
from jax.sharding import PartitionSpec as P

MESH = pl.DeviceIdType.MESH
F32 = jnp.float32
BF16 = jnp.bfloat16
NEG_BIG = -1e30
D = 2304
CHUNK = 768
TILE = 256
HEAD = 256
SPAN = 16
EXP_SCALE = 1.4426950408889634 * HEAD**-0.5
X_CHUNKS = ((0, 256), (256, 256), (512, 128), (640, 128))
NX = len(X_CHUNKS)


def nt_dot(a, b):
    return lax.dot_general(a, b, (((1,), (1,)), ((), ())), preferred_element_type=F32)


def kernel(x_ref, wq_ref, wk_ref, wv_ref, wo_ref, y_ref,
           x_buf, w_buf, kv_buf, q_buf, o_own, o_oth, o_rx, wo_own, wo_rx, y_acc, y_bf,
           m_sc, l_sc, acc_sc,
           xs, xr, ws, wr, os, orx, kvs, kvr, loc, ysem):
    tp = lax.axis_index("tp")
    r = lax.axis_index("sp")
    r1 = r + 1 - 2 * (r % 2)
    r2 = (r + 2) % 4
    peer_t = {"tp": 1 - tp, "sp": r}
    peer_x = {"tp": tp, "sp": r2}
    peer_c = {"tp": tp, "sp": r1}

    def block_id(rank, half):
        own = rank + tp * (7 - 2 * rank)
        return own if half == 0 else 7 - own

    def is_low(half):
        return tp == half

    def cond_x_send(half):
        return is_low(half) | (r >= 2)

    def cond_x_recv(half):
        return is_low(half) | (r < 2)

    def cond_c_send(half):
        return is_low(half) | (r % 2 == 1)

    def cond_c_recv(half):
        return is_low(half) | (r % 2 == 0)

    def remote(src, dst, send_sem, recv_sem, peer):
        return pltpu.make_async_remote_copy(src_ref=src, dst_ref=dst, send_sem=send_sem, recv_sem=recv_sem,
                                            device_id=peer, device_id_type=MESH)

    barrier = pltpu.get_barrier_semaphore()
    for peer in (peer_t, peer_x, peer_c):
        pl.semaphore_signal(barrier, inc=1, device_id=peer, device_id_type=MESH)
    pl.semaphore_wait(barrier, 3)

    def x_copy(c):
        row, n = X_CHUNKS[c]
        return remote(x_ref.at[pl.ds(row, n)], x_buf.at[1, pl.ds(row, n)], xs.at[c], xr.at[c], peer_t)

    for c in range(NX):
        x_copy(c).start()

    loads = [
        pltpu.make_async_copy(wk_ref, w_buf.at[pl.ds(0, 2)], loc.at[0]),
        pltpu.make_async_copy(wv_ref, w_buf.at[pl.ds(2, 2)], loc.at[1]),
        pltpu.make_async_copy(x_ref.at[pl.ds(0, 256)], x_buf.at[0, pl.ds(0, 256)], loc.at[2]),
        pltpu.make_async_copy(wq_ref, w_buf.at[pl.ds(4, 4)], loc.at[3]),
        pltpu.make_async_copy(x_ref.at[pl.ds(256, 512)], x_buf.at[0, pl.ds(256, 512)], loc.at[4]),
        pltpu.make_async_copy(wo_ref, wo_own, loc.at[5]),
    ]
    for copy in loads:
        copy.start()

    def kv_slices(half):
        return [(t, 0, TILE) for t in range(3)] if half == 0 else [(row // TILE, row % TILE, n) for row, n in X_CHUNKS]

    def kv_copy(half, c, kind):
        t, row, n = kv_slices(half)[c]
        src_rank = r2 if kind == 2 else r
        part = kv_buf.at[3 * block_id(src_rank, half) + t, :, pl.ds(row, n)]
        slot = (half * 3 + kind) * NX + c
        return remote(part, part, kvs.at[slot], kvr.at[slot], peer_x if kind == 0 else peer_c)

    def kv_recv_wait(half, c, kind):
        t, row, n = kv_slices(half)[c]
        src_rank = (r2, r1, 3 - r)[kind]
        part = kv_buf.at[3 * block_id(src_rank, half) + t, :, pl.ds(row, n)]
        slot = (half * 3 + kind) * NX + c
        remote(part, part, kvs.at[slot], kvr.at[slot], peer_x if kind == 0 else peer_c).wait_recv()

    def kv_send(half, c):
        @pl.when(cond_x_send(half))
        def _():
            kv_copy(half, c, 0).start()

        @pl.when(cond_c_send(half))
        def _():
            kv_copy(half, c, 1).start()

    def kv_forward(half, c):
        @pl.when(cond_x_recv(half))
        def _():
            kv_recv_wait(half, c, 0)
            kv_copy(half, c, 2).start()

    def kv_arrivals(half):
        for c in range(len(kv_slices(half))):
            @pl.when(cond_c_recv(half))
            def _():
                kv_recv_wait(half, c, 1)

            @pl.when(cond_x_recv(half))
            def _():
                kv_recv_wait(half, c, 2)

    def kv_drain(half):
        for c in range(len(kv_slices(half))):
            @pl.when(cond_x_send(half))
            def _():
                kv_copy(half, c, 0).wait_send()

            @pl.when(cond_c_send(half))
            def _():
                kv_copy(half, c, 1).wait_send()

            @pl.when(cond_x_recv(half))
            def _():
                kv_copy(half, c, 2).wait_send()

    def project_kv(half, row, n):
        tile = 3 * block_id(r, half) + row // TILE

        def step(j, _):
            kv_buf[tile, j, pl.ds(row % TILE, n)] = jnp.dot(
                x_buf[half, pl.ds(row, n)], w_buf[j], preferred_element_type=F32).astype(BF16)
            return 0

        lax.fori_loop(0, 4, step, 0)

    def project_q(half, row, n):
        def step(h, _):
            q_buf[half * 6 + (row // TILE) * 2 + h // 2, h % 2, pl.ds(row % TILE, n)] = jnp.dot(
                x_buf[half, pl.ds(row, n)], w_buf[4 + h], preferred_element_type=F32).astype(BF16)
            return 0

        lax.fori_loop(0, 4, step, 0)

    rows_i = lax.broadcasted_iota(jnp.int32, (TILE, TILE), 0)
    cols_i = lax.broadcasted_iota(jnp.int32, (TILE, TILE), 1)

    def attend(half, t, out):
        t_q = 3 * block_id(r, half) + t // 2
        g = t % 2
        q_at = half * 6 + t

        def lanes(p):
            total = p[:, :128]
            for i in range(1, p.shape[1] // 128):
                total = total + p[:, i * 128:(i + 1) * 128]
            return total

        for h in range(2):
            s = jnp.where(cols_i <= rows_i, nt_dot(q_buf[q_at, h], kv_buf[t_q, g]), NEG_BIG)
            m = jnp.max(s, axis=1, keepdims=True)
            p = jnp.exp2((s - m) * EXP_SCALE)
            m_sc[h] = jnp.broadcast_to(m, (TILE, 128))
            l_sc[h] = lanes(p)
            acc_sc[h] = jnp.dot(p.astype(BF16), kv_buf[t_q, 2 + g], preferred_element_type=F32)

        def update(h, tile, count, mask):
            q = q_buf[q_at, h]
            parts = [nt_dot(q, kv_buf[tile + i, g]) for i in range(count)]
            s = parts[0] if count == 1 else jnp.concatenate(parts, axis=1)
            if mask is not None:
                s = jnp.where(mask, s, NEG_BIG)
            m_old = m_sc[h][:, :1]
            m = jnp.maximum(m_old, jnp.max(s, axis=1, keepdims=True))
            p = jnp.exp2((s - m) * EXP_SCALE)
            alpha = jnp.exp2((m_old - m) * EXP_SCALE)
            m_sc[h] = jnp.broadcast_to(m, (TILE, 128))
            l_sc[h] = l_sc[h] * alpha + lanes(p)
            v = kv_buf[tile, 2 + g] if count == 1 else jnp.concatenate(
                [kv_buf[tile + i, 2 + g] for i in range(count)], axis=0)
            acc_sc[h] = acc_sc[h] * alpha + jnp.dot(p.astype(BF16), v, preferred_element_type=F32)

        @pl.when(t_q >= SPAN)
        def _():
            for h in range(2):
                update(h, t_q - SPAN, 1, cols_i > rows_i)

        n = jnp.where(t_q < SPAN - 1, t_q, SPAN - 1)
        low = t_q - n

        def step(i, _):
            for h in range(2):
                update(h, low + 2 * i, 2, None)
            return 0

        lax.fori_loop(0, n // 2, step, 0)

        @pl.when(n % 2 == 1)
        def _():
            for h in range(2):
                update(h, t_q - 1, 1, None)

        for h in range(2):
            total = jnp.sum(l_sc[h], axis=1, keepdims=True)
            out[t, :, h * HEAD:(h + 1) * HEAD] = (acc_sc[h] / total).astype(BF16)

    def o_copy(t):
        return remote(o_oth.at[t], o_rx.at[t], os.at[t], orx.at[t], peer_t)

    def wo_copy(kind):
        src = wo_ref.at[r] if kind == 0 else wo_rx.at[r2] if kind == 3 else wo_rx.at[r]
        dst = wo_rx.at[r2] if kind == 3 else wo_rx.at[r]
        peer = (peer_t, peer_x, peer_c, peer_c)[kind]
        return remote(src, dst, ws.at[kind], wr.at[kind], peer)

    def wo_recv_wait(kind):
        head = (r, r2, r1, 3 - r)[kind]
        remote(wo_rx.at[head], wo_rx.at[head], ws.at[kind], wr.at[kind], peer_t).wait_recv()

    for c in range(3):
        if c == 0:
            loads[0].wait()
            loads[1].wait()
            loads[2].wait()
        if c == 1:
            loads[4].wait()
        project_kv(0, c * TILE, TILE)
        kv_send(0, c)
        if c == 0:
            loads[3].wait()
        project_q(0, c * TILE, TILE)

    def other_rows(c):
        row, n = X_CHUNKS[c]
        x_copy(c).wait_recv()
        project_kv(1, row, n)
        kv_send(1, c)
        project_q(1, row, n)

    kv_forward(0, 0)
    other_rows(0)
    kv_forward(0, 1)
    kv_forward(0, 2)
    kv_arrivals(0)

    @pl.when(tp == 0)
    def _():
        def own(t, _):
            attend(0, t, o_own)
            return 0

        lax.fori_loop(0, 6, own, 0)

    other_rows(1)
    wo_copy(0).start()
    kv_forward(1, 0)
    other_rows(2)
    kv_forward(1, 1)
    other_rows(3)
    kv_forward(1, 2)
    kv_forward(1, 3)
    kv_arrivals(1)

    def other(t, _):
        attend(1, t, o_oth)
        o_copy(t).start()
        return 0

    lax.fori_loop(0, 6, other, 0)

    wo_recv_wait(0)
    wo_copy(1).start()
    wo_copy(2).start()

    @pl.when(tp == 1)
    def _():
        def own(t, _):
            attend(0, t, o_own)
            return 0

        lax.fori_loop(0, 6, own, 0)

    wo_recv_wait(1)
    wo_copy(3).start()
    loads[5].wait()

    def own_out(i, _):
        for j in range(3):
            cols = slice(j * CHUNK, (j + 1) * CHUNK)
            w = wo_own[:, :, cols].reshape(4 * HEAD, CHUNK)
            o = jnp.concatenate([o_own[2 * i], o_own[2 * i + 1]], axis=1)
            y_acc[i, :, cols] = jnp.dot(o, w, preferred_element_type=F32)
        return 0

    lax.fori_loop(0, 3, own_out, 0)
    wo_recv_wait(2)
    wo_recv_wait(3)

    def y_copy(i):
        return pltpu.make_async_copy(y_bf.at[pl.ds(i * TILE, TILE)], y_ref.at[pl.ds(i * TILE, TILE)], ysem.at[i])

    for i in range(3):
        for g in range(2):
            o_copy(2 * i + g).wait_recv()
            for j in range(3):
                cols = slice(j * CHUNK, (j + 1) * CHUNK)
                w = wo_rx[2 * g:2 * g + 2, :, cols].reshape(2 * HEAD, CHUNK)
                total = y_acc[i, :, cols] + jnp.dot(o_rx[2 * i + g], w, preferred_element_type=F32)
                if g == 0:
                    y_acc[i, :, cols] = total
                else:
                    y_bf[i * TILE:(i + 1) * TILE, cols] = total.astype(BF16)
        y_copy(i).start()

    for c in range(NX):
        x_copy(c).wait_send()
    kv_drain(0)
    kv_drain(1)
    for kind in range(4):
        wo_copy(kind).wait_send()
    for t in range(6):
        o_copy(t).wait_send()
    for i in range(3):
        y_copy(i).wait()


def solution(mesh):
    def local_attn(x, wq, wk, wv, wo):
        wq_t = wq.transpose(1, 0, 2)
        wk_t = wk.transpose(1, 0, 2)
        wv_t = wv.transpose(1, 0, 2)
        any_spec = pl.BlockSpec(memory_space=pl.ANY)
        return pl.pallas_call(
            kernel,
            out_shape=jax.ShapeDtypeStruct((CHUNK, D), BF16),
            in_specs=[any_spec] * 5,
            out_specs=any_spec,
            scratch_shapes=[
                pltpu.VMEM((2, CHUNK, D), BF16),
                pltpu.VMEM((8, D, HEAD), BF16),
                pltpu.VMEM((24, 4, TILE, HEAD), BF16),
                pltpu.VMEM((12, 2, TILE, HEAD), BF16),
                pltpu.VMEM((6, TILE, 2 * HEAD), BF16),
                pltpu.VMEM((6, TILE, 2 * HEAD), BF16),
                pltpu.VMEM((6, TILE, 2 * HEAD), BF16),
                pltpu.VMEM((4, HEAD, D), BF16),
                pltpu.VMEM((4, HEAD, D), BF16),
                pltpu.VMEM((3, TILE, D), F32),
                pltpu.VMEM((CHUNK, D), BF16),
                pltpu.VMEM((2, TILE, 128), F32),
                pltpu.VMEM((2, TILE, 128), F32),
                pltpu.VMEM((2, TILE, HEAD), F32),
                pltpu.SemaphoreType.DMA((NX,)),
                pltpu.SemaphoreType.DMA((NX,)),
                pltpu.SemaphoreType.DMA((4,)),
                pltpu.SemaphoreType.DMA((4,)),
                pltpu.SemaphoreType.DMA((6,)),
                pltpu.SemaphoreType.DMA((6,)),
                pltpu.SemaphoreType.DMA((6 * NX,)),
                pltpu.SemaphoreType.DMA((6 * NX,)),
                pltpu.SemaphoreType.DMA((6,)),
                pltpu.SemaphoreType.DMA((3,)),
            ],
            compiler_params=pltpu.CompilerParams(collective_id=0, has_side_effects=True, vmem_limit_bytes=66 * 1024 * 1024 - 2 * 1024 * 1024 - 65536),
            name="attn_block",
        )(x, wq_t, wk_t, wv_t, wo)

    return jax.shard_map(local_attn, mesh=mesh, in_specs=(P(("dp", "sp", "tp"), None), P(None, "tp", None), P(None, "tp", None), P(None, "tp", None), P("tp", None, None)), out_specs=P(("dp", "sp", "tp"), None), check_vma=False)
```

```python
import functools

import jax
import jax.numpy as jnp
from jax import lax
from jax.experimental import pallas as pl
from jax.experimental.pallas import tpu as pltpu
from jax.sharding import PartitionSpec as P

MESH = pl.DeviceIdType.MESH
F32 = jnp.float32
BF16 = jnp.bfloat16
NEG_BIG = -1e30
D = 2304
CHUNK = 768
TILE = 256
HEAD = 256
SPAN = 16
EXP_SCALE = 1.4426950408889634 * HEAD**-0.5
X_CHUNKS = ((0, 256), (256, 256), (512, 128), (640, 128))
NX = len(X_CHUNKS)


def nt_dot(a, b):
    return lax.dot_general(a, b, (((1,), (1,)), ((), ())), preferred_element_type=F32)


def kernel(x_ref, wq_ref, wk_ref, wv_ref, wo_ref, y_ref,
           x_buf, w_buf, kv_buf, q_buf, o_own, o_oth, o_rx, wo_own, wo_rx, y_acc, y_bf,
           m_sc, l_sc, acc_sc, s0_sc, sa_sc, sb_sc,
           xs, xr, ws, wr, os, orx, kvs, kvr, loc, ysem):
    tp = lax.axis_index("tp")
    r = lax.axis_index("sp")
    r1 = r + 1 - 2 * (r % 2)
    r2 = (r + 2) % 4
    peer_t = {"tp": 1 - tp, "sp": r}
    peer_x = {"tp": tp, "sp": r2}
    peer_c = {"tp": tp, "sp": r1}

    def block_id(rank, half):
        own = rank + tp * (7 - 2 * rank)
        return own if half == 0 else 7 - own

    def is_low(half):
        return tp == half

    def cond_x_send(half):
        return is_low(half) | (r >= 2)

    def cond_x_recv(half):
        return is_low(half) | (r < 2)

    def cond_c_send(half):
        return is_low(half) | (r % 2 == 1)

    def cond_c_recv(half):
        return is_low(half) | (r % 2 == 0)

    def remote(src, dst, send_sem, recv_sem, peer):
        return pltpu.make_async_remote_copy(src_ref=src, dst_ref=dst, send_sem=send_sem, recv_sem=recv_sem,
                                            device_id=peer, device_id_type=MESH)

    barrier = pltpu.get_barrier_semaphore()
    for peer in (peer_t, peer_x, peer_c):
        pl.semaphore_signal(barrier, inc=1, device_id=peer, device_id_type=MESH)
    pl.semaphore_wait(barrier, 3)

    def x_copy(c):
        row, n = X_CHUNKS[c]
        return remote(x_ref.at[pl.ds(row, n)], x_buf.at[1, pl.ds(row, n)], xs.at[c], xr.at[c], peer_t)

    for c in range(NX):
        x_copy(c).start()

    loads = [
        pltpu.make_async_copy(wk_ref, w_buf.at[pl.ds(0, 2)], loc.at[0]),
        pltpu.make_async_copy(wv_ref, w_buf.at[pl.ds(2, 2)], loc.at[1]),
        pltpu.make_async_copy(x_ref.at[pl.ds(0, 256)], x_buf.at[0, pl.ds(0, 256)], loc.at[2]),
        pltpu.make_async_copy(wq_ref, w_buf.at[pl.ds(4, 4)], loc.at[3]),
        pltpu.make_async_copy(x_ref.at[pl.ds(256, 512)], x_buf.at[0, pl.ds(256, 512)], loc.at[4]),
        pltpu.make_async_copy(wo_ref, wo_own, loc.at[5]),
    ]
    for copy in loads:
        copy.start()

    def kv_slices(half):
        return [(t, 0, TILE) for t in range(3)] if half == 0 else [(row // TILE, row % TILE, n) for row, n in X_CHUNKS]

    def kv_copy(half, c, kind):
        t, row, n = kv_slices(half)[c]
        src_rank = r2 if kind == 2 else r
        part = kv_buf.at[3 * block_id(src_rank, half) + t, :, pl.ds(row, n)]
        slot = (half * 3 + kind) * NX + c
        return remote(part, part, kvs.at[slot], kvr.at[slot], peer_x if kind == 0 else peer_c)

    def kv_recv_wait(half, c, kind):
        t, row, n = kv_slices(half)[c]
        src_rank = (r2, r1, 3 - r)[kind]
        part = kv_buf.at[3 * block_id(src_rank, half) + t, :, pl.ds(row, n)]
        slot = (half * 3 + kind) * NX + c
        remote(part, part, kvs.at[slot], kvr.at[slot], peer_x if kind == 0 else peer_c).wait_recv()

    def kv_send(half, c):
        @pl.when(cond_x_send(half))
        def _():
            kv_copy(half, c, 0).start()

        @pl.when(cond_c_send(half))
        def _():
            kv_copy(half, c, 1).start()

    def kv_forward(half, c):
        @pl.when(cond_x_recv(half))
        def _():
            kv_recv_wait(half, c, 0)
            kv_copy(half, c, 2).start()

    def kv_arrivals(half):
        for c in range(len(kv_slices(half))):
            @pl.when(cond_c_recv(half))
            def _():
                kv_recv_wait(half, c, 1)

            @pl.when(cond_x_recv(half))
            def _():
                kv_recv_wait(half, c, 2)

    def kv_drain(half):
        for c in range(len(kv_slices(half))):
            @pl.when(cond_x_send(half))
            def _():
                kv_copy(half, c, 0).wait_send()

            @pl.when(cond_c_send(half))
            def _():
                kv_copy(half, c, 1).wait_send()

            @pl.when(cond_x_recv(half))
            def _():
                kv_copy(half, c, 2).wait_send()

    def project_kv(half, row, n):
        tile = 3 * block_id(r, half) + row // TILE

        def step(j, _):
            kv_buf[tile, j, pl.ds(row % TILE, n)] = jnp.dot(
                x_buf[half, pl.ds(row, n)], w_buf[j], preferred_element_type=F32).astype(BF16)
            return 0

        lax.fori_loop(0, 4, step, 0)

    def project_q(half, row, n):
        def step(h, _):
            q_buf[half * 6 + (row // TILE) * 2 + h // 2, h % 2, pl.ds(row % TILE, n)] = jnp.dot(
                x_buf[half, pl.ds(row, n)], w_buf[4 + h], preferred_element_type=F32).astype(BF16)
            return 0

        lax.fori_loop(0, 4, step, 0)

    rows_i = lax.broadcasted_iota(jnp.int32, (TILE, TILE), 0)
    cols_i = lax.broadcasted_iota(jnp.int32, (TILE, TILE), 1)

    gap_i = cols_i - rows_i

    def attend(half, t, out):
        t_q = 3 * block_id(r, half) + t // 2
        g = t % 2
        q_at = half * 6 + t
        far = t_q >= SPAN
        n_full = jnp.where(t_q < SPAN - 1, t_q, SPAN - 1)
        low = t_q - n_full
        take = jnp.where(far, 1, jnp.where(t_q == 0, 0, 2 - t_q % 2))
        pairs = (n_full - take) // 2
        tile_b = jnp.where(far, t_q - SPAN, jnp.where(take == 2, t_q - 2, t_q))
        tile_c = jnp.where(take > 0, t_q - 1, t_q)
        gap_b = jnp.where(far, 0, jnp.where(take == 2, -TILE, TILE))
        gap_c = jnp.where(take > 0, -TILE, TILE)

        def pair_tiles(i):
            start = low + 2 * jnp.where(i < pairs, i, 0)
            return (start, start + 1)

        def scores(dst, tiles):
            for h in range(2):
                q = q_buf[q_at, h]
                for i, tile in enumerate(tiles):
                    dst[h, :, i * TILE:(i + 1) * TILE] = nt_dot(q, kv_buf[tile, g])

        def absorb(src, tiles, first):
            wide = 2 * len(tiles)
            for h in range(2):
                s = src[h]
                if first:
                    s = jnp.concatenate([
                        jnp.where(gap_i <= 0, s[:, :TILE], NEG_BIG),
                        jnp.where(gap_i > gap_b, s[:, TILE:2 * TILE], NEG_BIG),
                        jnp.where(gap_i > gap_c, s[:, 2 * TILE:], NEG_BIG)], axis=1)
                top = jnp.broadcast_to(jnp.max(s, axis=1, keepdims=True), (TILE, 128))
                m = top if first else jnp.maximum(m_sc[h], top)
                p = jnp.exp2((s - jnp.concatenate([m] * wide, axis=1)) * EXP_SCALE)
                total = p[:, :128]
                for i in range(1, wide):
                    total = total + p[:, i * 128:(i + 1) * 128]
                v = jnp.concatenate([kv_buf[tile, 2 + g] for tile in tiles], axis=0)
                o = jnp.dot(p.astype(BF16), v, preferred_element_type=F32)
                if first:
                    l_sc[h] = total
                    acc_sc[h] = o
                else:
                    alpha = jnp.exp2((m_sc[h] - m) * EXP_SCALE)
                    l_sc[h] = l_sc[h] * alpha + total
                    acc_sc[h] = acc_sc[h] * jnp.concatenate([alpha, alpha], axis=1) + o
                m_sc[h] = m

        first_tiles = (t_q, tile_b, tile_c)
        scores(s0_sc, first_tiles)
        scores(sa_sc, pair_tiles(0))
        absorb(s0_sc, first_tiles, True)

        def step(j, _):
            scores(sb_sc, pair_tiles(2 * j + 1))
            absorb(sa_sc, pair_tiles(2 * j), False)
            scores(sa_sc, pair_tiles(2 * j + 2))
            absorb(sb_sc, pair_tiles(2 * j + 1), False)
            return 0

        lax.fori_loop(0, pairs // 2, step, 0)

        @pl.when(pairs % 2 == 1)
        def _():
            absorb(sa_sc, pair_tiles(pairs - 1), False)

        for h in range(2):
            total = jnp.sum(l_sc[h], axis=1, keepdims=True)
            out[t, :, h * HEAD:(h + 1) * HEAD] = (acc_sc[h] / total).astype(BF16)

    def o_copy(t):
        return remote(o_oth.at[t], o_rx.at[t], os.at[t], orx.at[t], peer_t)

    def wo_copy(kind):
        src = wo_ref.at[r] if kind == 0 else wo_rx.at[r2] if kind == 3 else wo_rx.at[r]
        dst = wo_rx.at[r2] if kind == 3 else wo_rx.at[r]
        peer = (peer_t, peer_x, peer_c, peer_c)[kind]
        return remote(src, dst, ws.at[kind], wr.at[kind], peer)

    def wo_recv_wait(kind):
        head = (r, r2, r1, 3 - r)[kind]
        remote(wo_rx.at[head], wo_rx.at[head], ws.at[kind], wr.at[kind], peer_t).wait_recv()

    for c in range(3):
        if c == 0:
            loads[0].wait()
            loads[1].wait()
            loads[2].wait()
        if c == 1:
            loads[4].wait()
        project_kv(0, c * TILE, TILE)
        kv_send(0, c)
        if c == 0:
            loads[3].wait()
        project_q(0, c * TILE, TILE)

    def other_rows(c):
        row, n = X_CHUNKS[c]
        x_copy(c).wait_recv()
        project_kv(1, row, n)
        kv_send(1, c)
        project_q(1, row, n)

    kv_forward(0, 0)
    other_rows(0)
    kv_forward(0, 1)
    kv_forward(0, 2)
    kv_arrivals(0)

    @pl.when(tp == 0)
    def _():
        def own(t, _):
            attend(0, t, o_own)
            return 0

        lax.fori_loop(0, 6, own, 0)

    other_rows(1)
    wo_copy(0).start()
    kv_forward(1, 0)
    other_rows(2)
    kv_forward(1, 1)
    other_rows(3)
    kv_forward(1, 2)
    kv_forward(1, 3)
    kv_arrivals(1)

    def other(t, _):
        attend(1, t, o_oth)
        o_copy(t).start()
        return 0

    lax.fori_loop(0, 6, other, 0)

    wo_recv_wait(0)
    wo_copy(1).start()
    wo_copy(2).start()

    @pl.when(tp == 1)
    def _():
        def own(t, _):
            attend(0, t, o_own)
            return 0

        lax.fori_loop(0, 6, own, 0)

    wo_recv_wait(1)
    wo_copy(3).start()
    loads[5].wait()

    def own_out(i, _):
        for j in range(3):
            cols = slice(j * CHUNK, (j + 1) * CHUNK)
            w = wo_own[:, :, cols].reshape(4 * HEAD, CHUNK)
            o = jnp.concatenate([o_own[2 * i], o_own[2 * i + 1]], axis=1)
            y_acc[i, :, cols] = jnp.dot(o, w, preferred_element_type=F32)
        return 0

    lax.fori_loop(0, 3, own_out, 0)
    wo_recv_wait(2)
    wo_recv_wait(3)

    def y_copy(i):
        return pltpu.make_async_copy(y_bf.at[pl.ds(i * TILE, TILE)], y_ref.at[pl.ds(i * TILE, TILE)], ysem.at[i])

    for i in range(3):
        for g in range(2):
            o_copy(2 * i + g).wait_recv()
            for j in range(3):
                cols = slice(j * CHUNK, (j + 1) * CHUNK)
                w = wo_rx[2 * g:2 * g + 2, :, cols].reshape(2 * HEAD, CHUNK)
                total = y_acc[i, :, cols] + jnp.dot(o_rx[2 * i + g], w, preferred_element_type=F32)
                if g == 0:
                    y_acc[i, :, cols] = total
                else:
                    y_bf[i * TILE:(i + 1) * TILE, cols] = total.astype(BF16)
        y_copy(i).start()

    for c in range(NX):
        x_copy(c).wait_send()
    kv_drain(0)
    kv_drain(1)
    for kind in range(4):
        wo_copy(kind).wait_send()
    for t in range(6):
        o_copy(t).wait_send()
    for i in range(3):
        y_copy(i).wait()


def solution(mesh):
    def local_attn(x, wq, wk, wv, wo):
        wq_t = wq.transpose(1, 0, 2)
        wk_t = wk.transpose(1, 0, 2)
        wv_t = wv.transpose(1, 0, 2)
        any_spec = pl.BlockSpec(memory_space=pl.ANY)
        return pl.pallas_call(
            kernel,
            out_shape=jax.ShapeDtypeStruct((CHUNK, D), BF16),
            in_specs=[any_spec] * 5,
            out_specs=any_spec,
            scratch_shapes=[
                pltpu.VMEM((2, CHUNK, D), BF16),
                pltpu.VMEM((8, D, HEAD), BF16),
                pltpu.VMEM((24, 4, TILE, HEAD), BF16),
                pltpu.VMEM((12, 2, TILE, HEAD), BF16),
                pltpu.VMEM((6, TILE, 2 * HEAD), BF16),
                pltpu.VMEM((6, TILE, 2 * HEAD), BF16),
                pltpu.VMEM((6, TILE, 2 * HEAD), BF16),
                pltpu.VMEM((4, HEAD, D), BF16),
                pltpu.VMEM((4, HEAD, D), BF16),
                pltpu.VMEM((3, TILE, D), F32),
                pltpu.VMEM((CHUNK, D), BF16),
                pltpu.VMEM((2, TILE, 128), F32),
                pltpu.VMEM((2, TILE, 128), F32),
                pltpu.VMEM((2, TILE, HEAD), F32),
                pltpu.VMEM((2, TILE, 3 * TILE), F32),
                pltpu.VMEM((2, TILE, 2 * TILE), F32),
                pltpu.VMEM((2, TILE, 2 * TILE), F32),
                pltpu.SemaphoreType.DMA((NX,)),
                pltpu.SemaphoreType.DMA((NX,)),
                pltpu.SemaphoreType.DMA((4,)),
                pltpu.SemaphoreType.DMA((4,)),
                pltpu.SemaphoreType.DMA((6,)),
                pltpu.SemaphoreType.DMA((6,)),
                pltpu.SemaphoreType.DMA((6 * NX,)),
                pltpu.SemaphoreType.DMA((6 * NX,)),
                pltpu.SemaphoreType.DMA((6,)),
                pltpu.SemaphoreType.DMA((3,)),
            ],
            compiler_params=pltpu.CompilerParams(collective_id=0, has_side_effects=True, vmem_limit_bytes=66 * 1024 * 1024 - 2 * 1024 * 1024 - 65536),
            name="attn_block",
        )(x, wq_t, wk_t, wv_t, wo)

    return jax.shard_map(local_attn, mesh=mesh, in_specs=(P(("dp", "sp", "tp"), None), P(None, "tp", None), P(None, "tp", None), P(None, "tp", None), P("tp", None, None)), out_specs=P(("dp", "sp", "tp"), None), check_vma=False)
```

```python
import functools

import jax
import jax.numpy as jnp
from jax import lax
from jax.experimental import pallas as pl
from jax.experimental.pallas import tpu as pltpu
from jax.sharding import PartitionSpec as P

MESH = pl.DeviceIdType.MESH
F32 = jnp.float32
BF16 = jnp.bfloat16
NEG_BIG = -1e30
D = 2304
CHUNK = 768
TILE = 256
HEAD = 256
SPAN = 16
EXP_SCALE = 1.4426950408889634 * HEAD**-0.5
X_CHUNKS = ((0, 256), (256, 256), (512, 192), (704, 64))
NX = len(X_CHUNKS)
VMEM_LIMIT = 59 * 1024 * 1024


def nt_dot(a, b):
    return lax.dot_general(a, b, (((1,), (1,)), ((), ())), preferred_element_type=F32)


def kernel(x_ref, wq_ref, wk_ref, wv_ref, wo_ref, y_ref,
           x_buf, w_buf, kv_buf, q_buf, o_own, o_oth, o_rx, wo_own, wo_rx, y_acc,
           m_sc, l_sc, acc_sc, s0_sc, sa_sc, sb_sc,
           xs, xr, ws, wr, os, orx, kvs, kvr, loc):
    tp = lax.axis_index("tp")
    r = lax.axis_index("sp")
    r1 = r + 1 - 2 * (r % 2)
    r2 = (r + 2) % 4
    peer_t = {"tp": 1 - tp, "sp": r}
    peer_x = {"tp": tp, "sp": r2}
    peer_c = {"tp": tp, "sp": r1}

    def block_id(rank, half):
        own = rank + tp * (7 - 2 * rank)
        return own if half == 0 else 7 - own

    def is_low(half):
        return tp == half

    def cond_x_send(half):
        return is_low(half) | (r >= 2)

    def cond_x_recv(half):
        return is_low(half) | (r < 2)

    def cond_c_send(half):
        return is_low(half) | (r % 2 == 1)

    def cond_c_recv(half):
        return is_low(half) | (r % 2 == 0)

    def remote(src, dst, send_sem, recv_sem, peer):
        return pltpu.make_async_remote_copy(src_ref=src, dst_ref=dst, send_sem=send_sem, recv_sem=recv_sem,
                                            device_id=peer, device_id_type=MESH)

    barrier = pltpu.get_barrier_semaphore()
    for peer in (peer_t, peer_x, peer_c):
        pl.semaphore_signal(barrier, inc=1, device_id=peer, device_id_type=MESH)
    pl.semaphore_wait(barrier, 3)

    def x_copy(c):
        row, n = X_CHUNKS[c]
        return remote(x_ref.at[pl.ds(row, n)], x_buf.at[1, pl.ds(row, n)], xs.at[c], xr.at[c], peer_t)

    for c in range(NX):
        x_copy(c).start()

    loads = [
        pltpu.make_async_copy(wk_ref, w_buf.at[pl.ds(0, 2)], loc.at[0]),
        pltpu.make_async_copy(wv_ref, w_buf.at[pl.ds(2, 2)], loc.at[1]),
        pltpu.make_async_copy(x_ref.at[pl.ds(0, 256)], x_buf.at[0, pl.ds(0, 256)], loc.at[2]),
        pltpu.make_async_copy(wq_ref, w_buf.at[pl.ds(4, 4)], loc.at[3]),
        pltpu.make_async_copy(x_ref.at[pl.ds(256, 512)], x_buf.at[0, pl.ds(256, 512)], loc.at[4]),
        pltpu.make_async_copy(wo_ref, wo_own, loc.at[5]),
    ]
    for copy in loads:
        copy.start()

    def kv_slices(half):
        return [(t, 0, TILE) for t in range(3)] if half == 0 else [(row // TILE, row % TILE, n) for row, n in X_CHUNKS]

    def kv_copy(half, c, kind):
        t, row, n = kv_slices(half)[c]
        src_rank = r2 if kind == 2 else r
        part = kv_buf.at[3 * block_id(src_rank, half) + t, :, pl.ds(row, n)]
        slot = (half * 3 + kind) * NX + c
        return remote(part, part, kvs.at[slot], kvr.at[slot], peer_x if kind == 0 else peer_c)

    def kv_recv_wait(half, c, kind):
        t, row, n = kv_slices(half)[c]
        src_rank = (r2, r1, 3 - r)[kind]
        part = kv_buf.at[3 * block_id(src_rank, half) + t, :, pl.ds(row, n)]
        slot = (half * 3 + kind) * NX + c
        remote(part, part, kvs.at[slot], kvr.at[slot], peer_x if kind == 0 else peer_c).wait_recv()

    def kv_send(half, c):
        @pl.when(cond_x_send(half))
        def _():
            kv_copy(half, c, 0).start()

        @pl.when(cond_c_send(half))
        def _():
            kv_copy(half, c, 1).start()

    def kv_forward(half, c):
        @pl.when(cond_x_recv(half))
        def _():
            kv_recv_wait(half, c, 0)
            kv_copy(half, c, 2).start()

    def kv_arrivals(half):
        for c in range(len(kv_slices(half))):
            @pl.when(cond_c_recv(half))
            def _():
                kv_recv_wait(half, c, 1)

            @pl.when(cond_x_recv(half))
            def _():
                kv_recv_wait(half, c, 2)

    def kv_drain(half):
        for c in range(len(kv_slices(half))):
            @pl.when(cond_x_send(half))
            def _():
                kv_copy(half, c, 0).wait_send()

            @pl.when(cond_c_send(half))
            def _():
                kv_copy(half, c, 1).wait_send()

            @pl.when(cond_x_recv(half))
            def _():
                kv_copy(half, c, 2).wait_send()

    def project_kv(half, row, n):
        tile = 3 * block_id(r, half) + row // TILE

        def step(j, _):
            kv_buf[tile, j, pl.ds(row % TILE, n)] = jnp.dot(
                x_buf[half, pl.ds(row, n)], w_buf[j], preferred_element_type=F32).astype(BF16)
            return 0

        lax.fori_loop(0, 4, step, 0)

    def project_q(half, row, n):
        def step(h, _):
            q_buf[half * 6 + (row // TILE) * 2 + h // 2, h % 2, pl.ds(row % TILE, n)] = jnp.dot(
                x_buf[half, pl.ds(row, n)], w_buf[4 + h], preferred_element_type=F32).astype(BF16)
            return 0

        lax.fori_loop(0, 4, step, 0)

    rows_i = lax.broadcasted_iota(jnp.int32, (TILE, TILE), 0)
    cols_i = lax.broadcasted_iota(jnp.int32, (TILE, TILE), 1)

    gap_i = cols_i - rows_i

    def attend(half, t, out):
        t_q = 3 * block_id(r, half) + t // 2
        g = t % 2
        q_at = half * 6 + t
        far = t_q >= SPAN
        n_full = jnp.where(t_q < SPAN - 1, t_q, SPAN - 1)
        low = t_q - n_full
        take = jnp.where(far, 1, jnp.where(t_q == 0, 0, 2 - t_q % 2))
        pairs = (n_full - take) // 2
        tile_b = jnp.where(far, t_q - SPAN, jnp.where(take == 2, t_q - 2, t_q))
        tile_c = jnp.where(take > 0, t_q - 1, t_q)
        gap_b = jnp.where(far, 0, jnp.where(take == 2, -TILE, TILE))
        gap_c = jnp.where(take > 0, -TILE, TILE)

        def pair_tiles(i):
            start = low + 2 * jnp.where(i < pairs, i, 0)
            return (start, start + 1)

        def scores(dst, tiles):
            for h in range(2):
                q = q_buf[q_at, h]
                for i, tile in enumerate(tiles):
                    dst[h, :, i * TILE:(i + 1) * TILE] = nt_dot(q, kv_buf[tile, g])

        def absorb(src, tiles, first):
            wide = 2 * len(tiles)
            for h in range(2):
                s = src[h]
                if first:
                    s = jnp.concatenate([
                        jnp.where(gap_i <= 0, s[:, :TILE], NEG_BIG),
                        jnp.where(gap_i > gap_b, s[:, TILE:2 * TILE], NEG_BIG),
                        jnp.where(gap_i > gap_c, s[:, 2 * TILE:], NEG_BIG)], axis=1)
                top = jnp.broadcast_to(jnp.max(s, axis=1, keepdims=True), (TILE, 128))
                m = top if first else jnp.maximum(m_sc[h], top)
                p = jnp.exp2((s - jnp.concatenate([m] * wide, axis=1)) * EXP_SCALE)
                total = p[:, :128]
                for i in range(1, wide):
                    total = total + p[:, i * 128:(i + 1) * 128]
                v = jnp.concatenate([kv_buf[tile, 2 + g] for tile in tiles], axis=0)
                o = jnp.dot(p.astype(BF16), v, preferred_element_type=F32)
                if first:
                    l_sc[h] = total
                    acc_sc[h] = o
                else:
                    alpha = jnp.exp2((m_sc[h] - m) * EXP_SCALE)
                    l_sc[h] = l_sc[h] * alpha + total
                    acc_sc[h] = acc_sc[h] * jnp.concatenate([alpha, alpha], axis=1) + o
                m_sc[h] = m

        first_tiles = (t_q, tile_b, tile_c)
        scores(s0_sc, first_tiles)
        scores(sa_sc, pair_tiles(0))
        absorb(s0_sc, first_tiles, True)

        def step(j, _):
            scores(sb_sc, pair_tiles(2 * j + 1))
            absorb(sa_sc, pair_tiles(2 * j), False)
            scores(sa_sc, pair_tiles(2 * j + 2))
            absorb(sb_sc, pair_tiles(2 * j + 1), False)
            return 0

        lax.fori_loop(0, pairs // 2, step, 0)

        @pl.when(pairs % 2 == 1)
        def _():
            absorb(sa_sc, pair_tiles(pairs - 1), False)

        for h in range(2):
            total = jnp.sum(l_sc[h], axis=1, keepdims=True)
            out[t, :, h * HEAD:(h + 1) * HEAD] = (acc_sc[h] / total).astype(BF16)

    def o_copy(t):
        return remote(o_oth.at[t], o_rx.at[t], os.at[t], orx.at[t], peer_t)

    def wo_copy(kind):
        src = wo_ref.at[r] if kind == 0 else wo_rx.at[r2] if kind == 3 else wo_rx.at[r]
        dst = wo_rx.at[r2] if kind == 3 else wo_rx.at[r]
        peer = (peer_t, peer_x, peer_c, peer_c)[kind]
        return remote(src, dst, ws.at[kind], wr.at[kind], peer)

    def wo_recv_wait(kind):
        head = (r, r2, r1, 3 - r)[kind]
        remote(wo_rx.at[head], wo_rx.at[head], ws.at[kind], wr.at[kind], peer_t).wait_recv()

    for c in range(3):
        if c == 0:
            loads[0].wait()
            loads[1].wait()
            loads[2].wait()
        if c == 1:
            loads[4].wait()
        project_kv(0, c * TILE, TILE)
        kv_send(0, c)
        if c == 0:
            loads[3].wait()
        project_q(0, c * TILE, TILE)

    def other_rows(c):
        row, n = X_CHUNKS[c]
        x_copy(c).wait_recv()
        project_kv(1, row, n)
        kv_send(1, c)
        project_q(1, row, n)

    kv_forward(0, 0)
    other_rows(0)
    kv_forward(0, 1)
    kv_forward(0, 2)
    kv_arrivals(0)

    @pl.when(tp == 0)
    def _():
        def own(t, _):
            attend(0, t, o_own)
            return 0

        lax.fori_loop(0, 6, own, 0)

    other_rows(1)
    wo_copy(0).start()
    kv_forward(1, 0)
    other_rows(2)
    kv_forward(1, 1)
    other_rows(3)
    kv_forward(1, 2)
    kv_forward(1, 3)
    kv_arrivals(1)

    def other(t, _):
        attend(1, t, o_oth)
        o_copy(t).start()

        @pl.when(t == 3)
        def _():
            wo_recv_wait(0)
            wo_copy(1).start()
            wo_copy(2).start()

        return 0

    lax.fori_loop(0, 6, other, 0)

    @pl.when(tp == 1)
    def _():
        def own(t, _):
            attend(0, t, o_own)
            return 0

        lax.fori_loop(0, 6, own, 0)

    wo_recv_wait(1)
    wo_copy(3).start()
    loads[5].wait()

    def own_out(i, _):
        for j in range(3):
            cols = slice(j * CHUNK, (j + 1) * CHUNK)
            w = wo_own[:, :, cols].reshape(4 * HEAD, CHUNK)
            o = jnp.concatenate([o_own[2 * i], o_own[2 * i + 1]], axis=1)
            y_acc[i, :, cols] = jnp.dot(o, w, preferred_element_type=F32)
        return 0

    lax.fori_loop(0, 3, own_out, 0)
    wo_recv_wait(2)
    wo_recv_wait(3)

    for i in range(3):
        for g in range(2):
            o_copy(2 * i + g).wait_recv()
            for j in range(3):
                cols = slice(j * CHUNK, (j + 1) * CHUNK)
                w = wo_rx[2 * g:2 * g + 2, :, cols].reshape(2 * HEAD, CHUNK)
                total = y_acc[i, :, cols] + jnp.dot(o_rx[2 * i + g], w, preferred_element_type=F32)
                if g == 0:
                    y_acc[i, :, cols] = total
                else:
                    y_ref[i * TILE:(i + 1) * TILE, cols] = total.astype(BF16)

    for c in range(NX):
        x_copy(c).wait_send()
    kv_drain(0)
    kv_drain(1)
    for kind in range(4):
        wo_copy(kind).wait_send()
    for t in range(6):
        o_copy(t).wait_send()


def solution(mesh):
    def local_attn(x, wq, wk, wv, wo):
        wq_t = wq.transpose(1, 0, 2)
        wk_t = wk.transpose(1, 0, 2)
        wv_t = wv.transpose(1, 0, 2)
        any_spec = pl.BlockSpec(memory_space=pl.ANY)
        return pl.pallas_call(
            kernel,
            out_shape=pltpu.VMEM((CHUNK, D), BF16),
            in_specs=[any_spec] * 5,
            out_specs=pl.BlockSpec(memory_space=pltpu.VMEM),
            scratch_shapes=[
                pltpu.VMEM((2, CHUNK, D), BF16),
                pltpu.VMEM((8, D, HEAD), BF16),
                pltpu.VMEM((24, 4, TILE, HEAD), BF16),
                pltpu.VMEM((12, 2, TILE, HEAD), BF16),
                pltpu.VMEM((6, TILE, 2 * HEAD), BF16),
                pltpu.VMEM((6, TILE, 2 * HEAD), BF16),
                pltpu.VMEM((6, TILE, 2 * HEAD), BF16),
                pltpu.VMEM((4, HEAD, D), BF16),
                pltpu.VMEM((4, HEAD, D), BF16),
                pltpu.VMEM((3, TILE, D), F32),
                pltpu.VMEM((2, TILE, 128), F32),
                pltpu.VMEM((2, TILE, 128), F32),
                pltpu.VMEM((2, TILE, HEAD), F32),
                pltpu.VMEM((2, TILE, 3 * TILE), F32),
                pltpu.VMEM((2, TILE, 2 * TILE), F32),
                pltpu.VMEM((2, TILE, 2 * TILE), F32),
                pltpu.SemaphoreType.DMA((NX,)),
                pltpu.SemaphoreType.DMA((NX,)),
                pltpu.SemaphoreType.DMA((4,)),
                pltpu.SemaphoreType.DMA((4,)),
                pltpu.SemaphoreType.DMA((6,)),
                pltpu.SemaphoreType.DMA((6,)),
                pltpu.SemaphoreType.DMA((6 * NX,)),
                pltpu.SemaphoreType.DMA((6 * NX,)),
                pltpu.SemaphoreType.DMA((6,)),
            ],
            compiler_params=pltpu.CompilerParams(collective_id=0, has_side_effects=True, vmem_limit_bytes=VMEM_LIMIT),
            name="attn_block",
        )(x, wq_t, wk_t, wv_t, wo)

    return jax.shard_map(local_attn, mesh=mesh, in_specs=(P(("dp", "sp", "tp"), None), P(None, "tp", None), P(None, "tp", None), P(None, "tp", None), P("tp", None, None)), out_specs=P(("dp", "sp", "tp"), None), check_vma=False)
```

```python
import functools

import jax
import jax.numpy as jnp
from jax import lax
from jax.experimental import pallas as pl
from jax.experimental.pallas import tpu as pltpu
from jax.sharding import PartitionSpec as P

MESH = pl.DeviceIdType.MESH
F32 = jnp.float32
BF16 = jnp.bfloat16
NEG_BIG = -1e30
D = 2304
CHUNK = 768
TILE = 256
HEAD = 256
SPAN = 16
EXP_SCALE = 1.4426950408889634 * HEAD**-0.5
X_CHUNKS = ((0, 256), (256, 256), (512, 192), (704, 64))
HEAD_ROWS = 80
NX = len(X_CHUNKS)
VMEM_LIMIT = 59 * 1024 * 1024


def nt_dot(a, b):
    return lax.dot_general(a, b, (((1,), (1,)), ((), ())), preferred_element_type=F32)


def kernel(x_ref, x_head_ref, wq_ref, wk_ref, wv_ref, wo_ref, y_ref,
           x_buf, w_buf, kv_buf, q_buf, o_own, o_oth, o_rx, wo_own, wo_rx, y_acc,
           m_sc, l_sc, acc_sc, s0_sc, sa_sc, sb_sc,
           xs, xr, ws, wr, os, orx, kvs, kvr, loc):
    tp = lax.axis_index("tp")
    r = lax.axis_index("sp")
    r1 = r + 1 - 2 * (r % 2)
    r2 = (r + 2) % 4
    peer_t = {"tp": 1 - tp, "sp": r}
    peer_x = {"tp": tp, "sp": r2}
    peer_c = {"tp": tp, "sp": r1}

    def block_id(rank, half):
        own = rank + tp * (7 - 2 * rank)
        return own if half == 0 else 7 - own

    def is_low(half):
        return tp == half

    def cond_x_send(half):
        return is_low(half) | (r >= 2)

    def cond_x_recv(half):
        return is_low(half) | (r < 2)

    def cond_c_send(half):
        return is_low(half) | (r % 2 == 1)

    def cond_c_recv(half):
        return is_low(half) | (r % 2 == 0)

    def remote(src, dst, send_sem, recv_sem, peer):
        return pltpu.make_async_remote_copy(src_ref=src, dst_ref=dst, send_sem=send_sem, recv_sem=recv_sem,
                                            device_id=peer, device_id_type=MESH)

    barrier = pltpu.get_barrier_semaphore()
    for peer in (peer_t, peer_x, peer_c):
        pl.semaphore_signal(barrier, inc=1, device_id=peer, device_id_type=MESH)
    pl.semaphore_wait(barrier, 3)

    def x_copy(c):
        row, n = X_CHUNKS[c]
        if c == 0:
            row, n = row + HEAD_ROWS, n - HEAD_ROWS
        return remote(x_ref.at[pl.ds(row, n)], x_buf.at[1, pl.ds(row, n)], xs.at[c], xr.at[c], peer_t)

    for c in range(NX):
        x_copy(c).start()

    loads = [
        pltpu.make_async_copy(wk_ref, w_buf.at[pl.ds(0, 2)], loc.at[0]),
        pltpu.make_async_copy(wv_ref, w_buf.at[pl.ds(2, 2)], loc.at[1]),
        pltpu.make_async_copy(x_ref.at[pl.ds(0, 256)], x_buf.at[0, pl.ds(0, 256)], loc.at[2]),
        pltpu.make_async_copy(wq_ref, w_buf.at[pl.ds(4, 4)], loc.at[3]),
        pltpu.make_async_copy(x_ref.at[pl.ds(256, 512)], x_buf.at[0, pl.ds(256, 512)], loc.at[4]),
        pltpu.make_async_copy(wo_ref, wo_own, loc.at[5]),
        pltpu.make_async_copy(x_head_ref, x_buf.at[1, pl.ds(0, HEAD_ROWS)], loc.at[6]),
    ]
    for copy in loads:
        copy.start()

    def kv_slices(half):
        return [(t, 0, TILE) for t in range(3)] if half == 0 else [(row // TILE, row % TILE, n) for row, n in X_CHUNKS]

    def kv_copy(half, c, kind):
        t, row, n = kv_slices(half)[c]
        src_rank = r2 if kind == 2 else r
        part = kv_buf.at[3 * block_id(src_rank, half) + t, :, pl.ds(row, n)]
        slot = (half * 3 + kind) * NX + c
        return remote(part, part, kvs.at[slot], kvr.at[slot], peer_x if kind == 0 else peer_c)

    def kv_recv_wait(half, c, kind):
        t, row, n = kv_slices(half)[c]
        src_rank = (r2, r1, 3 - r)[kind]
        part = kv_buf.at[3 * block_id(src_rank, half) + t, :, pl.ds(row, n)]
        slot = (half * 3 + kind) * NX + c
        remote(part, part, kvs.at[slot], kvr.at[slot], peer_x if kind == 0 else peer_c).wait_recv()

    def kv_send(half, c):
        @pl.when(cond_x_send(half))
        def _():
            kv_copy(half, c, 0).start()

        @pl.when(cond_c_send(half))
        def _():
            kv_copy(half, c, 1).start()

    def kv_forward(half, c):
        @pl.when(cond_x_recv(half))
        def _():
            kv_recv_wait(half, c, 0)
            kv_copy(half, c, 2).start()

    def kv_arrivals(half):
        for c in range(len(kv_slices(half))):
            @pl.when(cond_c_recv(half))
            def _():
                kv_recv_wait(half, c, 1)

            @pl.when(cond_x_recv(half))
            def _():
                kv_recv_wait(half, c, 2)

    def kv_drain(half):
        for c in range(len(kv_slices(half))):
            @pl.when(cond_x_send(half))
            def _():
                kv_copy(half, c, 0).wait_send()

            @pl.when(cond_c_send(half))
            def _():
                kv_copy(half, c, 1).wait_send()

            @pl.when(cond_x_recv(half))
            def _():
                kv_copy(half, c, 2).wait_send()

    def project_kv(half, row, n):
        tile = 3 * block_id(r, half) + row // TILE

        def step(j, _):
            kv_buf[tile, j, pl.ds(row % TILE, n)] = jnp.dot(
                x_buf[half, pl.ds(row, n)], w_buf[j], preferred_element_type=F32).astype(BF16)
            return 0

        lax.fori_loop(0, 4, step, 0)

    def project_q(half, row, n):
        def step(h, _):
            q_buf[half * 6 + (row // TILE) * 2 + h // 2, h % 2, pl.ds(row % TILE, n)] = jnp.dot(
                x_buf[half, pl.ds(row, n)], w_buf[4 + h], preferred_element_type=F32).astype(BF16)
            return 0

        lax.fori_loop(0, 4, step, 0)

    rows_i = lax.broadcasted_iota(jnp.int32, (TILE, TILE), 0)
    cols_i = lax.broadcasted_iota(jnp.int32, (TILE, TILE), 1)

    gap_i = cols_i - rows_i

    def attend(half, t, out):
        t_q = 3 * block_id(r, half) + t // 2
        g = t % 2
        q_at = half * 6 + t
        far = t_q >= SPAN
        n_full = jnp.where(t_q < SPAN - 1, t_q, SPAN - 1)
        low = t_q - n_full
        take = jnp.where(far, 1, jnp.where(t_q == 0, 0, 2 - t_q % 2))
        pairs = (n_full - take) // 2
        tile_b = jnp.where(far, t_q - SPAN, jnp.where(take == 2, t_q - 2, t_q))
        tile_c = jnp.where(take > 0, t_q - 1, t_q)
        gap_b = jnp.where(far, 0, jnp.where(take == 2, -TILE, TILE))
        gap_c = jnp.where(take > 0, -TILE, TILE)

        def pair_tiles(i):
            start = low + 2 * jnp.where(i < pairs, i, 0)
            return (start, start + 1)

        def scores(dst, tiles):
            for h in range(2):
                q = q_buf[q_at, h]
                for i, tile in enumerate(tiles):
                    dst[h, :, i * TILE:(i + 1) * TILE] = nt_dot(q, kv_buf[tile, g])

        def absorb(src, tiles, first):
            wide = 2 * len(tiles)
            for h in range(2):
                s = src[h]
                if first:
                    s = jnp.concatenate([
                        jnp.where(gap_i <= 0, s[:, :TILE], NEG_BIG),
                        jnp.where(gap_i > gap_b, s[:, TILE:2 * TILE], NEG_BIG),
                        jnp.where(gap_i > gap_c, s[:, 2 * TILE:], NEG_BIG)], axis=1)
                top = jnp.broadcast_to(jnp.max(s, axis=1, keepdims=True), (TILE, 128))
                m = top if first else jnp.maximum(m_sc[h], top)
                p = jnp.exp2((s - jnp.concatenate([m] * wide, axis=1)) * EXP_SCALE)
                total = p[:, :128]
                for i in range(1, wide):
                    total = total + p[:, i * 128:(i + 1) * 128]
                v = jnp.concatenate([kv_buf[tile, 2 + g] for tile in tiles], axis=0)
                o = jnp.dot(p.astype(BF16), v, preferred_element_type=F32)
                if first:
                    l_sc[h] = total
                    acc_sc[h] = o
                else:
                    alpha = jnp.exp2((m_sc[h] - m) * EXP_SCALE)
                    l_sc[h] = l_sc[h] * alpha + total
                    acc_sc[h] = acc_sc[h] * jnp.concatenate([alpha, alpha], axis=1) + o
                m_sc[h] = m

        first_tiles = (t_q, tile_b, tile_c)
        scores(s0_sc, first_tiles)
        scores(sa_sc, pair_tiles(0))
        absorb(s0_sc, first_tiles, True)

        def step(j, _):
            scores(sb_sc, pair_tiles(2 * j + 1))
            absorb(sa_sc, pair_tiles(2 * j), False)
            scores(sa_sc, pair_tiles(2 * j + 2))
            absorb(sb_sc, pair_tiles(2 * j + 1), False)
            return 0

        lax.fori_loop(0, pairs // 2, step, 0)

        @pl.when(pairs % 2 == 1)
        def _():
            absorb(sa_sc, pair_tiles(pairs - 1), False)

        for h in range(2):
            total = jnp.sum(l_sc[h], axis=1, keepdims=True)
            out[t, :, h * HEAD:(h + 1) * HEAD] = (acc_sc[h] / total).astype(BF16)

    def o_copy(t):
        return remote(o_oth.at[t], o_rx.at[t], os.at[t], orx.at[t], peer_t)

    def wo_copy(kind):
        src = wo_ref.at[r] if kind == 0 else wo_rx.at[r2] if kind == 3 else wo_rx.at[r]
        dst = wo_rx.at[r2] if kind == 3 else wo_rx.at[r]
        peer = (peer_t, peer_x, peer_c, peer_c)[kind]
        return remote(src, dst, ws.at[kind], wr.at[kind], peer)

    def wo_recv_wait(kind):
        head = (r, r2, r1, 3 - r)[kind]
        remote(wo_rx.at[head], wo_rx.at[head], ws.at[kind], wr.at[kind], peer_t).wait_recv()

    for c in range(3):
        if c == 0:
            loads[0].wait()
            loads[1].wait()
            loads[2].wait()
        if c == 1:
            loads[4].wait()
        project_kv(0, c * TILE, TILE)
        kv_send(0, c)
        if c == 0:
            loads[3].wait()
        project_q(0, c * TILE, TILE)

    def other_rows(c):
        row, n = X_CHUNKS[c]
        if c == 0:
            loads[6].wait()
        x_copy(c).wait_recv()
        project_kv(1, row, n)
        kv_send(1, c)
        project_q(1, row, n)

    kv_forward(0, 0)
    other_rows(0)
    kv_forward(0, 1)
    kv_forward(0, 2)
    kv_arrivals(0)

    @pl.when(tp == 0)
    def _():
        def own(t, _):
            attend(0, t, o_own)
            return 0

        lax.fori_loop(0, 6, own, 0)

    other_rows(1)
    wo_copy(0).start()
    kv_forward(1, 0)
    other_rows(2)
    kv_forward(1, 1)
    other_rows(3)
    kv_forward(1, 2)
    kv_forward(1, 3)
    kv_arrivals(1)

    def other(t, _):
        attend(1, t, o_oth)
        o_copy(t).start()

        @pl.when(t == 3 + 2 * tp)
        def _():
            wo_recv_wait(0)
            wo_copy(1).start()
            wo_copy(2).start()

        return 0

    lax.fori_loop(0, 6, other, 0)

    @pl.when(tp == 1)
    def _():
        def own(t, _):
            attend(0, t, o_own)
            return 0

        lax.fori_loop(0, 6, own, 0)

    wo_recv_wait(1)
    wo_copy(3).start()
    loads[5].wait()

    def own_out(i, _):
        for j in range(3):
            cols = slice(j * CHUNK, (j + 1) * CHUNK)
            w = wo_own[:, :, cols].reshape(4 * HEAD, CHUNK)
            o = jnp.concatenate([o_own[2 * i], o_own[2 * i + 1]], axis=1)
            y_acc[i, :, cols] = jnp.dot(o, w, preferred_element_type=F32)
        return 0

    lax.fori_loop(0, 3, own_out, 0)
    wo_recv_wait(2)
    wo_recv_wait(3)

    for i in range(3):
        for g in range(2):
            o_copy(2 * i + g).wait_recv()
            for j in range(3):
                cols = slice(j * CHUNK, (j + 1) * CHUNK)
                w = wo_rx[2 * g:2 * g + 2, :, cols].reshape(2 * HEAD, CHUNK)
                total = y_acc[i, :, cols] + jnp.dot(o_rx[2 * i + g], w, preferred_element_type=F32)
                if g == 0:
                    y_acc[i, :, cols] = total
                else:
                    y_ref[i * TILE:(i + 1) * TILE, cols] = total.astype(BF16)

    for c in range(NX):
        x_copy(c).wait_send()
    kv_drain(0)
    kv_drain(1)
    for kind in range(4):
        wo_copy(kind).wait_send()
    for t in range(6):
        o_copy(t).wait_send()


def solution(mesh):
    def local_attn(x, wq, wk, wv, wo):
        x_head = lax.ppermute(x[:HEAD_ROWS], "tp", ((0, 1), (1, 0)))
        wq_t = wq.transpose(1, 0, 2)
        wk_t = wk.transpose(1, 0, 2)
        wv_t = wv.transpose(1, 0, 2)
        any_spec = pl.BlockSpec(memory_space=pl.ANY)
        return pl.pallas_call(
            kernel,
            out_shape=pltpu.VMEM((CHUNK, D), BF16),
            in_specs=[any_spec, pl.BlockSpec(memory_space=pltpu.HBM)] + [any_spec] * 4,
            out_specs=pl.BlockSpec(memory_space=pltpu.VMEM),
            scratch_shapes=[
                pltpu.VMEM((2, CHUNK, D), BF16),
                pltpu.VMEM((8, D, HEAD), BF16),
                pltpu.VMEM((24, 4, TILE, HEAD), BF16),
                pltpu.VMEM((12, 2, TILE, HEAD), BF16),
                pltpu.VMEM((6, TILE, 2 * HEAD), BF16),
                pltpu.VMEM((6, TILE, 2 * HEAD), BF16),
                pltpu.VMEM((6, TILE, 2 * HEAD), BF16),
                pltpu.VMEM((4, HEAD, D), BF16),
                pltpu.VMEM((4, HEAD, D), BF16),
                pltpu.VMEM((3, TILE, D), F32),
                pltpu.VMEM((2, TILE, 128), F32),
                pltpu.VMEM((2, TILE, 128), F32),
                pltpu.VMEM((2, TILE, HEAD), F32),
                pltpu.VMEM((2, TILE, 3 * TILE), F32),
                pltpu.VMEM((2, TILE, 2 * TILE), F32),
                pltpu.VMEM((2, TILE, 2 * TILE), F32),
                pltpu.SemaphoreType.DMA((NX,)),
                pltpu.SemaphoreType.DMA((NX,)),
                pltpu.SemaphoreType.DMA((4,)),
                pltpu.SemaphoreType.DMA((4,)),
                pltpu.SemaphoreType.DMA((6,)),
                pltpu.SemaphoreType.DMA((6,)),
                pltpu.SemaphoreType.DMA((6 * NX,)),
                pltpu.SemaphoreType.DMA((6 * NX,)),
                pltpu.SemaphoreType.DMA((7,)),
            ],
            compiler_params=pltpu.CompilerParams(collective_id=0, has_side_effects=True, vmem_limit_bytes=VMEM_LIMIT),
            name="attn_block",
        )(x, x_head, wq_t, wk_t, wv_t, wo)

    return jax.shard_map(local_attn, mesh=mesh, in_specs=(P(("dp", "sp", "tp"), None), P(None, "tp", None), P(None, "tp", None), P(None, "tp", None), P("tp", None, None)), out_specs=P(("dp", "sp", "tp"), None), check_vma=False)
```
